32 devices in a mesh: path: 8 (over y, x, core), mod: 4 (over z).
Axes of the slice: x: 2, y: 2, z: 4, core: 2. Of those that a mesh axis runs over, the one named last changes fastest.
Arguments:
- activations: bfloat16 [8, 512, 4096], P('path', 'mod'), may hold values from -6 to 6
- cotangent: bfloat16 [8, 512, 4096], P('path', 'mod'), may hold values from -6 to 6
- first_weight: bfloat16 [8, 4096, 4096], P('path', None, 'mod'), may hold values from -6 to 6
- second_weight: bfloat16 [8, 4096, 4096], P('path', None, 'mod'), may hold values from -6 to 6
- first_master: float32 [4, 4096, 4096], P(None, ('path', 'mod')), may hold values from -6 to 6
- second_master: float32 [4, 4096, 4096], P(None, ('path', 'mod')), may hold values from -6 to 6
- first_moment: float32 [4, 4096, 4096], P(None, ('path', 'mod')), may hold values from -3 to 3
- second_moment: float32 [4, 4096, 4096], P(None, ('path', 'mod')), may hold values from -3 to 3
- routing: int32 [8, 2], replicated, may hold values from 0 to 3, as said below
Outputs:
- first_result: bfloat16 [8, 4096, 4096], P('path', None, 'mod')
- second_result: bfloat16 [8, 4096, 4096], P('path', None, 'mod')
The draws below stay inside these ranges and needn't reach their ends.
Inputs may be any that keep to these rules, and one draw needn't show every extreme that they name: `routing`: for each of the two levels, every one of the 4 modules is taken by at least one path.
All inputs are finite; a program needn't handle non-finite values.
Results may differ from the reference program's by a relative error of at most 0.0045.
Values may be sent and summed in bfloat16 or wider, within the bound.
A program may use at most 192 MiB of HBM per device.

```python
import jax
import jax.numpy as jnp
from jax import lax

D = 4096
MODS = 4
TOK = 512
PATHS = 8


def draw_routing(key, part):
    subkeys = jax.random.split(jax.random.fold_in(key, 17), 4)
    columns = []
    for level_index in range(2):
        picked = jax.random.randint(subkeys[level_index], (PATHS,), 0, MODS)
        shuffled = jax.random.permutation(subkeys[level_index + 2], PATHS)
        picked = picked.at[shuffled[:MODS]].set(jnp.arange(MODS))
        columns.append(picked)
    return jnp.stack(columns, axis=1).astype(jnp.int32)


def block_levels(key, dims, pieces, least, high):
    def one(axis_at, parts):
        steps = jax.random.uniform(jax.random.fold_in(jax.random.fold_in(key, 6), axis_at), (parts,), jnp.float32, least / len(pieces), high / len(pieces))
        return jnp.repeat(jnp.exp(steps), dims[axis_at] // parts).reshape((-1,) + (1,) * (len(dims) - axis_at - 1))

    loudness = one(*pieces[0])
    for cut in pieces[1:]:
        loudness = loudness * one(*cut)
    return loudness


def bell_draw(own_key, shape, deviation, most, cuts=(), dtype=jnp.bfloat16):
    level = block_levels(own_key, shape, cuts, -0.22, 0.18) if cuts else 1.0
    entries = jax.random.normal(own_key, shape, jnp.float32) * deviation * level
    return jnp.minimum(jnp.maximum(entries, -most), most).astype(dtype)


def setup_inputs(seed: int = 0) -> dict:
    keys = jax.random.split(jax.random.key(seed), 10)
    return {
        "activations": bell_draw(keys[0], (PATHS, TOK, D), 1.0, 6.0, ((0, 8), (1, 4))),
        "cotangent": bell_draw(keys[1], (PATHS, TOK, D), 1.0, 6.0, ((0, 8), (1, 4))),
        "first_weight": bell_draw(keys[2], (PATHS, D, D), 1.0, 6.0, ((0, 8), (2, 4))),
        "second_weight": bell_draw(keys[3], (PATHS, D, D), 1.0, 6.0, ((0, 8), (2, 4))),
        "first_master": bell_draw(keys[4], (MODS, D, D), 1.0, 6.0, ((1, 32),), jnp.float32),
        "second_master": bell_draw(keys[5], (MODS, D, D), 1.0, 6.0, ((1, 32),), jnp.float32),
        "first_moment": bell_draw(keys[6], (MODS, D, D), 0.5, 3.0, ((1, 32),), jnp.float32),
        "second_moment": bell_draw(keys[7], (MODS, D, D), 0.5, 3.0, ((1, 32),), jnp.float32),
        "routing": draw_routing(jax.random.fold_in(keys[9], 71), 0),
    }


inner_rate = 1.0
outer_rate = 0.7
momentum_decay = 0.9


def path_update(operands):
    inputs_full, upstream, weight_in, weight_out = operands
    scale = D ** -0.5
    pre = jnp.dot(inputs_full, weight_in, preferred_element_type=jnp.float32) * scale
    hidden = jax.nn.silu(pre).astype(jnp.bfloat16)
    grad_hidden = jnp.dot(upstream, weight_out, preferred_element_type=jnp.float32) * scale
    grad_out = lax.dot_general(upstream, hidden, (((0,), (0,)), ((), ())), preferred_element_type=jnp.float32) * scale
    sigma = jax.nn.sigmoid(pre)
    grad_pre = (grad_hidden * sigma * (1.0 + pre * (1.0 - sigma))).astype(jnp.bfloat16)
    grad_in = lax.dot_general(inputs_full, grad_pre, (((0,), (0,)), ((), ())), preferred_element_type=jnp.float32) * scale
    trained_in = (weight_in.astype(jnp.float32) - inner_rate * grad_in).astype(jnp.bfloat16)
    trained_out = (weight_out.astype(jnp.float32) - inner_rate * grad_out).astype(jnp.bfloat16)
    return trained_in, trained_out


def reference(activations, cotangent, first_weight, second_weight, first_master, second_master, first_moment, second_moment, routing):
    trained_in, trained_out = lax.map(path_update, (activations, cotangent, first_weight, second_weight))
    module_ids = jnp.arange(MODS).astype(jnp.int32)
    results = []
    levels = ((trained_in, first_master, first_moment), (trained_out, second_master, second_moment))
    for level_index in range(2):
        trained, master, moment = levels[level_index]
        onehot = (routing[:, level_index][:, None] == module_ids[None, :]).astype(jnp.float32)

        def accumulate(summed, operands):
            weights_row, trained_one = operands
            return summed + weights_row[:, None, None] * trained_one.astype(jnp.float32)[None], None

        summed, _ = lax.scan(accumulate, jnp.zeros(master.shape, jnp.float32), (onehot, trained))
        path_total = jnp.sum(onehot, axis=0)[:, None, None]
        outer = master - summed / path_total
        moment_new = momentum_decay * moment + outer
        renewed = (master - outer_rate * (outer + momentum_decay * moment_new)).astype(jnp.bfloat16)
        results.append(renewed[routing[:, level_index]])
    return results[0], results[1]
```

```python
import functools

import jax
import jax.numpy as jnp
from jax import lax
from jax.experimental import pallas as pl
from jax.experimental.pallas import tpu as pltpu
from jax.sharding import PartitionSpec as P

inner_rate = 1.0
outer_rate = 0.7
momentum_decay = 0.9

mean_factor = outer_rate * (1.0 + momentum_decay)
master_factor = 1.0 - mean_factor
moment_factor = -outer_rate * momentum_decay * momentum_decay

ANY = pl.BlockSpec(memory_space=pl.ANY)
SMEM = pl.BlockSpec(memory_space=pltpu.SMEM)
f32 = jnp.float32
bf16 = jnp.bfloat16


def remote(src, dst, send_sem, recv_sem, where):
    return pltpu.make_async_remote_copy(
        src_ref=src,
        dst_ref=dst,
        send_sem=send_sem,
        recv_sem=recv_sem,
        device_id=where,
        device_id_type=pl.DeviceIdType.MESH,
    )


def aligned(start, size):
    return pl.ds(pl.multiple_of(start, size), size)


def round_kernel(
    paths,
    groups,
    act,
    cot,
    w1,
    w2,
    m1,
    m2,
    u1,
    u2,
    coef,
    routing,
    r1,
    r2,
    b1,
    b2,
    c1,
    c2,
    arr1,
    actv,
    cotv,
    slv,
    w1v,
    w2v,
    arr2,
    hid,
    pre,
    gpre,
    acc,
    fresh,
    chunk,
    base,
    mbuf,
    ubuf,
    obuf,
    zs,
    zr,
    ss,
    sr,
    ws,
    wr,
    hs,
    hr,
    fs,
    fr,
    ts,
    tr,
    bs,
    br,
    os,
    orr,
    loc,
    outloc,
    pipe,
):
    p = lax.axis_index("path")
    z = lax.axis_index("mod")
    tokens, depth = act.shape
    cols = w1.shape[1]
    rows = depth // paths
    sub = m1.shape[1]
    modules = m1.shape[0]
    all_tokens = tokens * groups
    tile = min(cols, 256)
    scale = depth ** (-0.5)
    half = paths // 2
    partner = p + 1 - 2 * lax.rem(p, 2)
    last = groups - 1

    def ahead(step):
        return lax.rem(p + step, paths)

    def behind(step):
        return lax.rem(p + paths - step, paths)

    bufs = (actv, cotv, slv)

    def hop(i, d, s, src, block):
        to = lax.rem(z + 1, groups) if d == 0 else lax.rem(z + last, groups)
        return remote(src, bufs[i].at[block], zs.at[i, d, s], zr.at[i, d, s], (p, to))

    def can_send(d):
        return z < last if d == 0 else z > 0

    def own_send(i, d, src, also=None):
        cond = can_send(d)
        if also is not None:
            cond = jnp.logical_and(cond, also)

        @pl.when(cond)
        def _():
            hop(i, d, 0, src, z).start()

    def block_of(d, s):
        return z - s if d == 0 else z + s

    def present(d, s):
        return z >= s if d == 0 else z + s <= last

    def relay_step(i, s):
        for d in (0, 1):
            block = block_of(d, s)

            @pl.when(present(d, s))
            def _():
                hop(i, d, s - 1, bufs[i].at[block], block).wait_recv()

            @pl.when(jnp.logical_and(present(d, s), can_send(d)))
            def _():
                hop(i, d, s, bufs[i].at[block], block).start()

    def for_blocks(s, work):
        for d in (0, 1):

            @pl.when(present(d, s))
            def _():
                work(block_of(d, s))

    def relay_finish(i):
        for s in range(groups):
            for d in (0, 1):

                @pl.when(jnp.logical_and(present(d, s), can_send(d)))
                def _():
                    block = block_of(d, s)
                    hop(i, d, s, bufs[i].at[block], block).wait_send()

    def next_own(s):
        own_send(1, 0, cot, z == s)
        own_send(1, 1, cot, z == last - s)

    for d in (0, 1):
        own_send(0, d, act)
    next_own(0)

    def slice_copy(step):
        to = ahead(step)
        return remote(
            cot.at[:, aligned(to * rows, rows)], slv.at[z, p], ss.at[step], sr.at[step], (to, z)
        )

    def raw_copy(step):
        to = ahead(step)
        return remote(
            w2.at[aligned(to * rows, rows), :], arr2.at[p], ws.at[step], wr.at[step], (to, z)
        )

    for step in range(1, paths):
        slice_copy(step).start()
    for step in range(1, paths):
        raw_copy(step).start()

    load_act = pltpu.make_async_copy(act, actv.at[z], loc.at[0])
    load_cot = pltpu.make_async_copy(cot, cotv.at[z], loc.at[1])
    load_w1 = pltpu.make_async_copy(w1, w1v, loc.at[2])
    load_w2 = pltpu.make_async_copy(w2, w2v, loc.at[3])
    load_slice = pltpu.make_async_copy(
        cot.at[:, aligned(p * rows, rows)], slv.at[z, p], loc.at[4]
    )
    load_raw = pltpu.make_async_copy(w2.at[aligned(p * rows, rows), :], arr2.at[p], loc.at[5])
    loads = (load_act, load_w1, load_cot, load_w2, load_slice, load_raw)
    for load in loads:
        load.start()

    band = mbuf.shape[1]
    per = sub // band
    for m_ref, u_ref, b_ref in ((m2, u2, b2), (m1, u1, b1)):
        count = modules * per

        def where(i):
            return lax.div(i, per), aligned(lax.rem(i, per) * band, band)

        def fetch(i, slot):
            m, r = where(i)
            return (
                pltpu.make_async_copy(m_ref.at[m, r, :], mbuf.at[slot], pipe.at[0, slot]),
                pltpu.make_async_copy(u_ref.at[m, r, :], ubuf.at[slot], pipe.at[1, slot]),
            )

        def put(i, slot):
            m, r = where(i)
            return pltpu.make_async_copy(obuf.at[slot], b_ref.at[m, r, :], pipe.at[2, slot])

        for c in fetch(0, 0):
            c.start()

        def base_step(i, carry):
            slot = lax.rem(i, 2)
            for c in fetch(i, slot):
                c.wait()

            @pl.when(i + 1 < count)
            def _():
                for c in fetch(i + 1, 1 - slot):
                    c.start()

            @pl.when(i >= 2)
            def _():
                put(i - 2, slot).wait()

            obuf[slot] = (master_factor * mbuf[slot] + moment_factor * ubuf[slot]).astype(bf16)
            put(i, slot).start()
            return carry

        lax.fori_loop(0, count, base_step, 0)
        for i in range(max(0, count - 2), count):
            put(i, i % 2).wait()

    for load in loads:
        load.wait()

    def forward(block):
        here = aligned(block * tokens, tokens)

        def column(n, carry):
            at = aligned(n * tile, tile)
            value = jnp.dot(actv[block], w1v[:, at], preferred_element_type=f32) * scale
            pre[here, at] = value
            hid[p, here, at] = jax.nn.silu(value).astype(bf16)
            return carry

        lax.fori_loop(0, cols // tile, column, 0)

    forward(z)
    for s in range(1, groups):
        relay_step(0, s)
        next_own(s)
        for_blocks(s, forward)

    def hidden_copy(j):
        to = partner if j == 0 else ahead(2 * j)
        return remote(hid.at[p], hid.at[p], hs.at[j], hr.at[j], (to, z))

    def hidden_arrival(j):
        q = partner if j == 0 else behind(2 * j)
        return remote(hid.at[q], hid.at[q], hs.at[j], hr.at[j], (partner, z))

    def hidden_onward(j):
        q = behind(2 * j)
        return remote(hid.at[q], hid.at[q], fs.at[j], fr.at[j], (partner, z))

    def hidden_second(j):
        q = lax.rem(partner + paths - 2 * j, paths)
        return remote(hid.at[q], hid.at[q], fs.at[j], fr.at[j], (partner, z))

    for j in range(half - 1, -1, -1):
        hidden_copy(j).start()

    def backward(block):
        here = aligned(block * tokens, tokens)

        def column(n, carry):
            at = aligned(n * tile, tile)
            value = jnp.dot(cotv[block], w2v[:, at], preferred_element_type=f32) * scale
            before = pre[here, at]
            sigma = jax.nn.sigmoid(before)
            gpre[here, at] = (value * sigma * (1.0 + before * (1.0 - sigma))).astype(bf16)
            return carry

        lax.fori_loop(0, cols // tile, column, 0)

    backward(z)
    for s in range(1, groups):
        relay_step(1, s)
        if s == last:
            for step in range(1, paths):
                q = behind(step)
                remote(
                    slv.at[z, q], slv.at[z, q], ss.at[step], sr.at[step], (ahead(step), z)
                ).wait_recv()
            for d in (0, 1):
                own_send(2, d, slv.at[z])
        for_blocks(s, backward)

    def trained_copy(step):
        to = ahead(step)
        return remote(
            w1v.at[aligned(to * rows, rows), :], arr1.at[p], ts.at[step], tr.at[step], (to, z)
        )

    own_trained = pltpu.make_async_copy(w1v.at[aligned(p * rows, rows), :], arr1.at[p], loc.at[6])

    for step in list(range(1, paths)) + [0]:
        q = ahead(step)
        here = aligned(q * rows, rows)
        lhs = actv[:, :, here].reshape(all_tokens, rows)

        def column(n, carry):
            at = aligned(n * tile, tile)
            grad = lax.dot_general(
                lhs, gpre[:, at], (((0,), (0,)), ((), ())), preferred_element_type=f32
            )
            w1v[here, at] = (w1v[here, at].astype(f32) - inner_rate * (grad * scale)).astype(bf16)
            return carry

        lax.fori_loop(0, cols // tile, column, 0)
        if step == 0:
            own_trained.start()
        else:
            trained_copy(step).start()

    for j in range(1, half):
        hidden_arrival(j).wait_recv()
        hidden_onward(j).start()

    def base_copy(level, step):
        b, c = ((b1, c1), (b2, c2))[level]
        to = lax.rem(z + step, groups)
        return remote(
            b.at[:, :, aligned(to * cols, cols)],
            c.at[:, aligned(z * sub, sub), :],
            bs.at[level, step],
            br.at[level, step],
            (p, to),
        )

    for s in range(1, groups):
        relay_step(2, s)
        if s == max(1, last - 1):
            for level in (1, 0):
                for step in range(1, groups):
                    base_copy(level, step).start()

    hidden_arrival(0).wait_recv()
    for j in range(1, half):
        hidden_second(j).wait_recv()
    for step in range(1, paths):
        q = behind(step)
        remote(
            arr2.at[q], arr2.at[q], ws.at[step], wr.at[step], (ahead(step), z)
        ).wait_recv()

    results = (r1, r2)

    def staged(level, st, q, here):
        if level == 1:
            return arr2.at[q, here, :]
        return w2v.at[aligned((st * paths + q) * sub, sub), :]

    def out_copy(level, st, step):
        j = lax.rem(z + groups - st, groups)
        to = ahead(step)
        src = staged(level, st, to, aligned(j * sub, sub))
        dst = results[level].at[aligned(p * rows + j * sub, sub), :]
        if step == 0:
            return pltpu.make_async_copy(src, dst, outloc.at[level, st])
        return remote(src, dst, os.at[level, st, step], orr.at[level, st, step], (to, z))

    def out_arrival(level, st, step):
        j = lax.rem(z + groups - st, groups)
        q = behind(step)
        dst = results[level].at[aligned(q * rows + j * sub, sub), :]
        return remote(
            dst, dst, os.at[level, st, step], orr.at[level, st, step], (ahead(step), z)
        )

    def combine(level, st, trained):
        j = lax.rem(z + groups - st, groups)
        here = aligned(j * sub, sub)
        b, c = ((b1, c1), (b2, c2))[level]
        acc[...] = jnp.zeros_like(acc)

        def add(q, carry):
            value = trained(q, here)
            for m in range(modules):
                acc[m] = acc[m] + coef[level, m, q] * value
            return carry

        lax.fori_loop(0, paths, add, 0)
        if st == 0:
            src = b.at[:, :, aligned(z * cols, cols)]
        else:
            src = c.at[:, here, :]
            remote(
                src, src, bs.at[level, st], br.at[level, st], (p, lax.rem(z + st, groups))
            ).wait_recv()
        load = pltpu.make_async_copy(src, base, loc.at[7])
        load.start()
        load.wait()
        for m in range(modules):
            fresh[m] = (base[m].astype(f32) + acc[m]).astype(bf16)

        def place(q, carry):
            value = fresh[routing[q, level]]
            if level == 1:
                arr2[q, here, :] = value
            else:
                w2v[aligned((st * paths + q) * sub, sub), :] = value
            return carry

        lax.fori_loop(0, paths, place, 0)
        for step in list(range(1, paths)) + [0]:
            out_copy(level, st, step).start()

    def train_second(q, carry):
        lhs = slv[:, q, :, :].reshape(all_tokens, rows)

        def column(n, carry):
            at = aligned(n * tile, tile)
            grad = lax.dot_general(
                lhs, hid[q, :, at], (((0,), (0,)), ((), ())), preferred_element_type=f32
            )
            raw = arr2[q, :, at].astype(f32)
            arr2[q, :, at] = (raw - inner_rate * (grad * scale)).astype(bf16)
            return carry

        return lax.fori_loop(0, cols // tile, column, carry)

    lax.fori_loop(0, paths, train_second, 0)

    def second(q, here):
        return arr2[q, here, :].astype(f32)

    for st in range(groups):
        combine(1, st, second)

    own_trained.wait()
    for step in range(1, paths):
        q = behind(step)
        remote(
            arr1.at[q], arr1.at[q], ts.at[step], tr.at[step], (ahead(step), z)
        ).wait_recv()

    def first(q, here):
        return chunk[q].astype(f32)

    for st in range(groups):
        j = lax.rem(z + groups - st, groups)
        load = pltpu.make_async_copy(arr1.at[:, aligned(j * sub, sub), :], chunk, loc.at[8])
        load.start()
        load.wait()
        combine(0, st, first)

    for i in range(3):
        relay_finish(i)
    for step in range(1, paths):
        slice_copy(step).wait_send()
        raw_copy(step).wait_send()
        trained_copy(step).wait_send()
    for j in range(half):
        hidden_copy(j).wait_send()
    for j in range(1, half):
        hidden_onward(j).wait_send()
    for level in (1, 0):
        for step in range(1, groups):
            base_copy(level, step).wait_send()
        for st in range(groups):
            out_copy(level, st, 0).wait()
            for step in range(1, paths):
                out_copy(level, st, step).wait_send()
                out_arrival(level, st, step).wait_recv()


def body(
    activations,
    cotangent,
    first_weight,
    second_weight,
    first_master,
    second_master,
    first_moment,
    second_moment,
    routing,
):
    paths = lax.axis_size("path")
    groups = lax.axis_size("mod")
    act = activations[0]
    cot = cotangent[0]
    w1 = first_weight[0]
    w2 = second_weight[0]
    tokens, depth = act.shape
    cols = w1.shape[1]
    rows = depth // paths
    modules, sub, _ = first_master.shape
    band = min(sub, 32)

    onehot = (jnp.transpose(routing)[:, None, :] == jnp.arange(modules)[None, :, None]).astype(f32)
    coef = onehot * (mean_factor / jnp.sum(onehot, axis=2, keepdims=True))

    dma = pltpu.SemaphoreType.DMA
    result = jax.ShapeDtypeStruct((depth, cols), bf16)
    based = jax.ShapeDtypeStruct((modules, sub, depth), bf16)
    moved = jax.ShapeDtypeStruct((modules, rows, cols), bf16)
    outs = pl.pallas_call(
        functools.partial(round_kernel, paths, groups),
        out_shape=(
            result,
            result,
            based,
            based,
            moved,
            moved,
            jax.ShapeDtypeStruct((paths, rows, cols), bf16),
        ),
        in_specs=[ANY] * 8 + [SMEM] * 2,
        out_specs=[ANY] * 7,
        scratch_shapes=[
            pltpu.VMEM((groups, tokens, depth), bf16),
            pltpu.VMEM((groups, tokens, depth), bf16),
            pltpu.VMEM((groups, paths, tokens, rows), bf16),
            pltpu.VMEM((depth, cols), bf16),
            pltpu.VMEM((depth, cols), bf16),
            pltpu.VMEM((paths, rows, cols), bf16),
            pltpu.VMEM((paths, tokens * groups, cols), bf16),
            pltpu.VMEM((tokens * groups, cols), f32),
            pltpu.VMEM((tokens * groups, cols), bf16),
            pltpu.VMEM((modules, sub, cols), f32),
            pltpu.VMEM((modules, sub, cols), bf16),
            pltpu.VMEM((paths, sub, cols), bf16),
            pltpu.VMEM((modules, sub, cols), bf16),
            pltpu.VMEM((2, band, depth), f32),
            pltpu.VMEM((2, band, depth), f32),
            pltpu.VMEM((2, band, depth), bf16),
            dma((3, 2, groups)),
            dma((3, 2, groups)),
            dma((paths,)),
            dma((paths,)),
            dma((paths,)),
            dma((paths,)),
            dma((paths // 2,)),
            dma((paths // 2,)),
            dma((paths // 2,)),
            dma((paths // 2,)),
            dma((paths,)),
            dma((paths,)),
            dma((2, groups)),
            dma((2, groups)),
            dma((2, groups, paths)),
            dma((2, groups, paths)),
            dma((9,)),
            dma((2, groups)),
            dma((3, 2)),
        ],
        compiler_params=pltpu.CompilerParams(
            has_side_effects=True, vmem_limit_bytes=67_000_000
        ),
        name="outer_round",
    )(
        act,
        cot,
        w1,
        w2,
        first_master,
        second_master,
        first_moment,
        second_moment,
        coef,
        routing,
    )
    return (outs[0][None], outs[1][None])


def solution(mesh):
    return jax.shard_map(
        body,
        mesh=mesh,
        in_specs=(
            P("path", "mod", None),
            P("path", "mod", None),
            P("path", None, "mod"),
            P("path", None, "mod"),
            P(None, ("path", "mod"), None),
            P(None, ("path", "mod"), None),
            P(None, ("path", "mod"), None),
            P(None, ("path", "mod"), None),
            P(),
        ),
        out_specs=(P("path", None, "mod"), P("path", None, "mod")),
        check_vma=False,
    )
```

```python
import functools

import jax
import jax.numpy as jnp
from jax import lax
from jax.experimental import pallas as pl
from jax.experimental.pallas import tpu as pltpu
from jax.sharding import PartitionSpec as P

inner_rate = 1.0
outer_rate = 0.7
momentum_decay = 0.9

mean_factor = outer_rate * (1.0 + momentum_decay)
master_factor = 1.0 - mean_factor
moment_factor = -outer_rate * momentum_decay * momentum_decay

ANY = pl.BlockSpec(memory_space=pl.ANY)
SMEM = pl.BlockSpec(memory_space=pltpu.SMEM)
MESH = pl.DeviceIdType.MESH
f32 = jnp.float32
bf16 = jnp.bfloat16


def remote(src, dst, send_sem, recv_sem, where):
    return pltpu.make_async_remote_copy(
        src_ref=src,
        dst_ref=dst,
        send_sem=send_sem,
        recv_sem=recv_sem,
        device_id=where,
        device_id_type=pl.DeviceIdType.MESH,
    )


def aligned(start, size):
    return pl.ds(pl.multiple_of(start, size), size)


def round_kernel(
    paths,
    groups,
    act,
    cot,
    w1,
    w2,
    m1,
    m2,
    u1,
    u2,
    routing,
    r1,
    r2,
    b1,
    b2,
    c1,
    c2,
    arr1,
    actv,
    cotv,
    slv,
    w1v,
    w2v,
    arr2,
    hid,
    pre,
    gpre,
    acc,
    fresh,
    chunk,
    base,
    mbuf,
    ubuf,
    obuf,
    zs,
    zr,
    ss,
    sr,
    ws,
    wr,
    hs,
    hr,
    fs,
    fr,
    ts,
    tr,
    bs,
    br,
    os,
    orr,
    loc,
    outloc,
    pipe,
    done,
):
    p = lax.axis_index("path")
    z = lax.axis_index("mod")
    tokens, depth = act.shape
    cols = w1.shape[1]
    rows = depth // paths
    sub = m1.shape[1]
    modules = m1.shape[0]
    all_tokens = tokens * groups
    tile = min(cols, 256)
    scale = depth ** (-0.5)
    half = paths // 2
    partner = p + 1 - 2 * lax.rem(p, 2)
    last = groups - 1

    def ahead(step):
        return lax.rem(p + step, paths)

    def behind(step):
        return lax.rem(p + paths - step, paths)

    bufs = (actv, cotv, slv)

    def hop(i, d, s, src, block):
        to = lax.rem(z + 1, groups) if d == 0 else lax.rem(z + last, groups)
        return remote(src, bufs[i].at[block], zs.at[i, d, s], zr.at[i, d, s], (p, to))

    def can_send(d):
        return z < last if d == 0 else z > 0

    def own_send(i, d, src):
        @pl.when(can_send(d))
        def _():
            hop(i, d, 0, src, z).start()

    def block_of(d, s):
        return z - s if d == 0 else z + s

    def present(d, s):
        return z >= s if d == 0 else z + s <= last

    def relay_step(i, s):
        for d in (0, 1):
            block = block_of(d, s)

            @pl.when(present(d, s))
            def _():
                hop(i, d, s - 1, bufs[i].at[block], block).wait_recv()

            @pl.when(jnp.logical_and(present(d, s), can_send(d)))
            def _():
                hop(i, d, s, bufs[i].at[block], block).start()

    def for_blocks(s, work):
        for d in (0, 1):

            @pl.when(present(d, s))
            def _():
                work(block_of(d, s))

    def relay_finish(i):
        for s in range(groups):
            for d in (0, 1):

                @pl.when(jnp.logical_and(present(d, s), can_send(d)))
                def _():
                    block = block_of(d, s)
                    hop(i, d, s, bufs[i].at[block], block).wait_send()

    barrier = pltpu.get_barrier_semaphore()
    for step in range(1, paths):
        pl.semaphore_signal(barrier, inc=1, device_id=(ahead(step), z), device_id_type=MESH)
    for step in range(1, groups):
        pl.semaphore_signal(
            barrier, inc=1, device_id=(p, lax.rem(z + step, groups)), device_id_type=MESH
        )
    pl.semaphore_wait(barrier, paths + groups - 2)

    for i, own in enumerate((act, cot)):
        for d in (0, 1):
            own_send(i, d, own)

    def slice_copy(step):
        to = ahead(step)
        return remote(
            cot.at[:, aligned(to * rows, rows)], slv.at[z, p], ss.at[step], sr.at[step], (to, z)
        )

    def raw_copy(step):
        to = ahead(step)
        return remote(
            w2.at[aligned(to * rows, rows), :], arr2.at[p], ws.at[step], wr.at[step], (to, z)
        )

    for step in range(1, paths):
        slice_copy(step).start()
    for step in range(1, paths):
        raw_copy(step).start()

    load_act = pltpu.make_async_copy(act, actv.at[z], loc.at[0])
    load_cot = pltpu.make_async_copy(cot, cotv.at[z], loc.at[1])
    load_w1 = pltpu.make_async_copy(w1, w1v, loc.at[2])
    load_w2 = pltpu.make_async_copy(w2, w2v, loc.at[3])
    load_slice = pltpu.make_async_copy(
        cot.at[:, aligned(p * rows, rows)], slv.at[z, p], loc.at[4]
    )
    load_raw = pltpu.make_async_copy(w2.at[aligned(p * rows, rows), :], arr2.at[p], loc.at[5])
    loads = (load_act, load_w1, load_cot, load_w2, load_slice, load_raw)
    for load in loads:
        load.start()

    band = mbuf.shape[1]
    per = sub // band
    count = modules * per // 2

    def base_part(part):
        level, first_band = (1, 1, 0, 0)[part], (part % 2) * count
        m_ref, u_ref, b_ref = ((m1, u1, b1), (m2, u2, b2))[level]

        def where(i):
            i = first_band + i
            return lax.div(i, per), aligned(lax.rem(i, per) * band, band)

        def fetch(i, slot):
            m, r = where(i)
            return (
                pltpu.make_async_copy(m_ref.at[m, r, :], mbuf.at[slot], pipe.at[0, slot]),
                pltpu.make_async_copy(u_ref.at[m, r, :], ubuf.at[slot], pipe.at[1, slot]),
            )

        def put(i, slot):
            m, r = where(i)
            return pltpu.make_async_copy(obuf.at[slot], b_ref.at[m, r, :], pipe.at[2, slot])

        for copy in fetch(0, 0):
            copy.start()

        def base_step(i, carry):
            slot = lax.rem(i, 2)
            for copy in fetch(i, slot):
                copy.wait()

            @pl.when(i + 1 < count)
            def _():
                for copy in fetch(i + 1, 1 - slot):
                    copy.start()

            @pl.when(i >= 2)
            def _():
                put(i - 2, slot).wait()

            obuf[slot] = (master_factor * mbuf[slot] + moment_factor * ubuf[slot]).astype(bf16)
            put(i, slot).start()
            return carry

        with jax.named_scope("base"):
            lax.fori_loop(0, count, base_step, 0)
            for i in range(max(0, count - 2), count):
                put(i, i % 2).wait()

    for load in loads:
        load.wait()

    def forward(block):
        here = aligned(block * tokens, tokens)

        def column(n, carry):
            at = aligned(n * tile, tile)
            value = jnp.dot(actv[block], w1v[:, at], preferred_element_type=f32) * scale
            pre[here, at] = value
            hid[p, here, at] = jax.nn.silu(value).astype(bf16)
            return carry

        lax.fori_loop(0, cols // tile, column, 0)

    forward(z)
    parts = list(range(4))
    for s in range(1, groups):
        if parts:
            base_part(parts.pop(0))
        relay_step(0, s)
        for_blocks(s, forward)

    def hidden_copy(j):
        to = partner if j == 0 else ahead(2 * j)
        return remote(hid.at[p], hid.at[p], hs.at[j], hr.at[j], (to, z))

    def hidden_arrival(j):
        q = partner if j == 0 else behind(2 * j)
        return remote(hid.at[q], hid.at[q], hs.at[j], hr.at[j], (partner, z))

    def hidden_onward(j):
        q = behind(2 * j)
        return remote(hid.at[q], hid.at[q], fs.at[j], fr.at[j], (partner, z))

    def hidden_second(j):
        q = lax.rem(partner + paths - 2 * j, paths)
        return remote(hid.at[q], hid.at[q], fs.at[j], fr.at[j], (partner, z))

    for j in range(half - 1, -1, -1):
        hidden_copy(j).start()

    def backward(block):
        here = aligned(block * tokens, tokens)

        def column(n, carry):
            at = aligned(n * tile, tile)
            value = jnp.dot(cotv[block], w2v[:, at], preferred_element_type=f32) * scale
            before = pre[here, at]
            sigma = jax.nn.sigmoid(before)
            gpre[here, at] = (value * sigma * (1.0 + before * (1.0 - sigma))).astype(bf16)
            return carry

        lax.fori_loop(0, cols // tile, column, 0)

    backward(z)
    for s in range(1, groups):
        if parts:
            base_part(parts.pop(0))
        relay_step(1, s)
        if s == last:
            for step in range(1, paths):
                q = behind(step)
                remote(
                    slv.at[z, q], slv.at[z, q], ss.at[step], sr.at[step], (ahead(step), z)
                ).wait_recv()
            for d in (0, 1):
                own_send(2, d, slv.at[z])
        for_blocks(s, backward)

    def trained_copy(step):
        to = ahead(step)
        return remote(
            w1v.at[aligned(to * rows, rows), :], arr1.at[p], ts.at[step], tr.at[step], (to, z)
        )

    own_trained = pltpu.make_async_copy(w1v.at[aligned(p * rows, rows), :], arr1.at[p], loc.at[6])

    for step in list(range(1, paths)) + [0]:
        q = ahead(step)
        here = aligned(q * rows, rows)
        lhs = actv[:, :, here].reshape(all_tokens, rows)

        def column(n, carry):
            at = aligned(n * tile, tile)
            grad = lax.dot_general(
                lhs, gpre[:, at], (((0,), (0,)), ((), ())), preferred_element_type=f32
            )
            w1v[here, at] = (w1v[here, at].astype(f32) - inner_rate * (grad * scale)).astype(bf16)
            return carry

        lax.fori_loop(0, cols // tile, column, 0)
        if step == 0:
            own_trained.start()
        else:
            trained_copy(step).start()

    def base_copy(level, step):
        b, c = ((b1, c1), (b2, c2))[level]
        to = lax.rem(z + step, groups)
        return remote(
            b.at[:, :, aligned(to * cols, cols)],
            c.at[:, aligned(z * sub, sub), :],
            bs.at[level, step],
            br.at[level, step],
            (p, to),
        )

    while parts:
        base_part(parts.pop(0))
    for s in range(1, groups):
        relay_step(2, s)
        if s == 1:
            for j in range(1, half):
                hidden_arrival(j).wait_recv()
                hidden_onward(j).start()

    def inner(at):
        return jnp.logical_and(at > 0, at < last)

    def base_sends(early):
        for step in range(1, groups):
            within = jnp.logical_and(inner(z), inner(lax.rem(z + step, groups)))

            @pl.when(within if early else jnp.logical_not(within))
            def _():
                base_copy(1, step).start()

    base_sends(True)
    for step in range(1, groups):
        pl.semaphore_signal(
            done, inc=1, device_id=(p, lax.rem(z + step, groups)), device_id_type=MESH
        )
    with jax.named_scope("column"):
        pl.semaphore_wait(done, groups - 1)
    base_sends(False)

    hidden_arrival(0).wait_recv()
    for j in range(1, half):
        hidden_second(j).wait_recv()
    for step in range(1, paths):
        q = behind(step)
        remote(
            arr2.at[q], arr2.at[q], ws.at[step], wr.at[step], (ahead(step), z)
        ).wait_recv()

    results = (r1, r2)

    def staged(level, st, q, here):
        if level == 1:
            return arr2.at[q, here, :]
        return w2v.at[aligned((st * paths + q) * sub, sub), :]

    def out_copy(level, st, step):
        j = lax.rem(z + groups - st, groups)
        to = ahead(step)
        src = staged(level, st, to, aligned(j * sub, sub))
        dst = results[level].at[aligned(p * rows + j * sub, sub), :]
        if step == 0:
            return pltpu.make_async_copy(src, dst, outloc.at[level, st])
        return remote(src, dst, os.at[level, st, step], orr.at[level, st, step], (to, z))

    def out_arrival(level, st, step):
        j = lax.rem(z + groups - st, groups)
        q = behind(step)
        dst = results[level].at[aligned(q * rows + j * sub, sub), :]
        return remote(
            dst, dst, os.at[level, st, step], orr.at[level, st, step], (ahead(step), z)
        )

    def factor(level, m):
        taken = jnp.int32(0)
        for q in range(paths):
            taken = taken + jnp.where(routing[q, level] == m, 1, 0)
        value = jnp.float32(mean_factor)
        for k in range(2, paths + 1):
            value = jnp.where(taken == k, jnp.float32(mean_factor / k), value)
        return value

    factors = [[factor(level, m) for m in range(modules)] for level in range(2)]

    def combine(level, st, trained):
        j = lax.rem(z + groups - st, groups)
        here = aligned(j * sub, sub)
        b, c = ((b1, c1), (b2, c2))[level]
        acc[...] = jnp.zeros_like(acc)

        def add(q, carry):
            value = trained(q, here)
            for m in range(modules):
                weight = jnp.where(routing[q, level] == m, factors[level][m], 0.0)
                acc[m] = acc[m] + weight * value
            return carry

        lax.fori_loop(0, paths, add, 0)
        if st == 0:
            src = b.at[:, :, aligned(z * cols, cols)]
        else:
            src = c.at[:, here, :]
            remote(
                src, src, bs.at[level, st], br.at[level, st], (p, lax.rem(z + st, groups))
            ).wait_recv()
        load = pltpu.make_async_copy(src, base, loc.at[7])
        load.start()
        load.wait()
        for m in range(modules):
            fresh[m] = (base[m].astype(f32) + acc[m]).astype(bf16)

        def place(q, carry):
            value = fresh[routing[q, level]]
            if level == 1:
                arr2[q, here, :] = value
            else:
                w2v[aligned((st * paths + q) * sub, sub), :] = value
            return carry

        lax.fori_loop(0, paths, place, 0)
        for step in list(range(1, paths)) + [0]:
            out_copy(level, st, step).start()

    def train_second(q, carry):
        lhs = slv[:, q, :, :].reshape(all_tokens, rows)

        def column(n, carry):
            at = aligned(n * tile, tile)
            grad = lax.dot_general(
                lhs, hid[q, :, at], (((0,), (0,)), ((), ())), preferred_element_type=f32
            )
            raw = arr2[q, :, at].astype(f32)
            arr2[q, :, at] = (raw - inner_rate * (grad * scale)).astype(bf16)
            return carry

        return lax.fori_loop(0, cols // tile, column, carry)

    lax.fori_loop(0, paths, train_second, 0)

    def second(q, here):
        return arr2[q, here, :].astype(f32)

    for st in range(groups):
        combine(1, st, second)
    for step in range(1, groups):
        base_copy(0, step).start()

    own_trained.wait()
    for step in range(1, paths):
        q = behind(step)
        remote(
            arr1.at[q], arr1.at[q], ts.at[step], tr.at[step], (ahead(step), z)
        ).wait_recv()

    def first(q, here):
        return chunk[q].astype(f32)

    for st in range(groups):
        j = lax.rem(z + groups - st, groups)
        load = pltpu.make_async_copy(arr1.at[:, aligned(j * sub, sub), :], chunk, loc.at[8])
        load.start()
        load.wait()
        combine(0, st, first)

    for i in range(3):
        relay_finish(i)
    for step in range(1, paths):
        slice_copy(step).wait_send()
        raw_copy(step).wait_send()
        trained_copy(step).wait_send()
    for j in range(half):
        hidden_copy(j).wait_send()
    for j in range(1, half):
        hidden_onward(j).wait_send()
    for level in (1, 0):
        for step in range(1, groups):
            base_copy(level, step).wait_send()
        for st in range(groups):
            out_copy(level, st, 0).wait()
            for step in range(1, paths):
                out_copy(level, st, step).wait_send()
                out_arrival(level, st, step).wait_recv()


def deliver_kernel(block, a0, a1, o0, o1, buf, sem):
    copies = []
    for level, (a, o) in enumerate(((a0, o0), (a1, o1))):
        for i in range(a.shape[0] // block):
            here = pl.ds(i * block, block)
            slot = buf.at[level, here, :]
            copies.append(
                (
                    pltpu.make_async_copy(a.at[here, :], slot, sem.at[level, i, 0]),
                    pltpu.make_async_copy(slot, o.at[here, :], sem.at[level, i, 1]),
                )
            )
    for fetch, _ in copies:
        fetch.start()
    for fetch, put in copies:
        fetch.wait()
        put.start()
    for _, put in copies:
        put.wait()


def deliver(a0, a1):
    depth, cols = a0.shape
    block = depth // 8
    return pl.pallas_call(
        functools.partial(deliver_kernel, block),
        out_shape=(jax.ShapeDtypeStruct(a0.shape, a0.dtype),) * 2,
        in_specs=[ANY] * 2,
        out_specs=[ANY] * 2,
        scratch_shapes=[
            pltpu.VMEM((2, depth, cols), a0.dtype),
            pltpu.SemaphoreType.DMA((2, depth // block, 2)),
        ],
        compiler_params=pltpu.CompilerParams(vmem_limit_bytes=67_000_000),
        name="deliver",
    )(a0, a1)


def body(
    activations,
    cotangent,
    first_weight,
    second_weight,
    first_master,
    second_master,
    first_moment,
    second_moment,
    routing,
):
    paths = lax.axis_size("path")
    groups = lax.axis_size("mod")
    act = activations[0]
    cot = cotangent[0]
    w1 = first_weight[0]
    w2 = second_weight[0]
    tokens, depth = act.shape
    cols = w1.shape[1]
    rows = depth // paths
    modules, sub, _ = first_master.shape
    band = min(sub, 32)

    dma = pltpu.SemaphoreType.DMA
    result = jax.ShapeDtypeStruct((depth, cols), bf16)
    based = jax.ShapeDtypeStruct((modules, sub, depth), bf16)
    moved = jax.ShapeDtypeStruct((modules, rows, cols), bf16)
    outs = pl.pallas_call(
        functools.partial(round_kernel, paths, groups),
        out_shape=(
            result,
            result,
            based,
            based,
            moved,
            moved,
            jax.ShapeDtypeStruct((paths, rows, cols), bf16),
        ),
        in_specs=[ANY] * 8 + [SMEM],
        out_specs=[ANY] * 7,
        scratch_shapes=[
            pltpu.VMEM((groups, tokens, depth), bf16),
            pltpu.VMEM((groups, tokens, depth), bf16),
            pltpu.VMEM((groups, paths, tokens, rows), bf16),
            pltpu.VMEM((depth, cols), bf16),
            pltpu.VMEM((depth, cols), bf16),
            pltpu.VMEM((paths, rows, cols), bf16),
            pltpu.VMEM((paths, tokens * groups, cols), bf16),
            pltpu.VMEM((tokens * groups, cols), f32),
            pltpu.VMEM((tokens * groups, cols), bf16),
            pltpu.VMEM((modules, sub, cols), f32),
            pltpu.VMEM((modules, sub, cols), bf16),
            pltpu.VMEM((paths, sub, cols), bf16),
            pltpu.VMEM((modules, sub, cols), bf16),
            pltpu.VMEM((2, band, depth), f32),
            pltpu.VMEM((2, band, depth), f32),
            pltpu.VMEM((2, band, depth), bf16),
            dma((3, 2, groups)),
            dma((3, 2, groups)),
            dma((paths,)),
            dma((paths,)),
            dma((paths,)),
            dma((paths,)),
            dma((paths // 2,)),
            dma((paths // 2,)),
            dma((paths // 2,)),
            dma((paths // 2,)),
            dma((paths,)),
            dma((paths,)),
            dma((2, groups)),
            dma((2, groups)),
            dma((2, groups, paths)),
            dma((2, groups, paths)),
            dma((9,)),
            dma((2, groups)),
            dma((3, 2)),
            pltpu.SemaphoreType.REGULAR,
        ],
        compiler_params=pltpu.CompilerParams(
            has_side_effects=True, vmem_limit_bytes=67_000_000, collective_id=0
        ),
        name="outer_round",
    )(
        act,
        cot,
        w1,
        w2,
        first_master,
        second_master,
        first_moment,
        second_moment,
        routing,
    )
    first_back, second_back = deliver(outs[0], outs[1])
    return (first_back[None], second_back[None])


def solution(mesh):
    return jax.shard_map(
        body,
        mesh=mesh,
        in_specs=(
            P("path", "mod", None),
            P("path", "mod", None),
            P("path", None, "mod"),
            P("path", None, "mod"),
            P(None, ("path", "mod"), None),
            P(None, ("path", "mod"), None),
            P(None, ("path", "mod"), None),
            P(None, ("path", "mod"), None),
            P(),
        ),
        out_specs=(P("path", None, "mod"), P("path", None, "mod")),
        check_vma=False,
    )
```

```python
import functools

import jax
import jax.numpy as jnp
from jax import lax
from jax.experimental import pallas as pl
from jax.experimental.pallas import tpu as pltpu
from jax.sharding import PartitionSpec as P

inner_rate = 1.0
outer_rate = 0.7
momentum_decay = 0.9

mean_factor = outer_rate * (1.0 + momentum_decay)
master_factor = 1.0 - mean_factor
moment_factor = -outer_rate * momentum_decay * momentum_decay

ANY = pl.BlockSpec(memory_space=pl.ANY)
SMEM = pl.BlockSpec(memory_space=pltpu.SMEM)
MESH = pl.DeviceIdType.MESH
f32 = jnp.float32
bf16 = jnp.bfloat16


def remote(src, dst, send_sem, recv_sem, where):
    return pltpu.make_async_remote_copy(
        src_ref=src,
        dst_ref=dst,
        send_sem=send_sem,
        recv_sem=recv_sem,
        device_id=where,
        device_id_type=pl.DeviceIdType.MESH,
    )


def aligned(start, size):
    return pl.ds(pl.multiple_of(start, size), size)


def round_kernel(
    paths,
    groups,
    act,
    cot,
    w1,
    w2,
    m1,
    m2,
    u1,
    u2,
    routing,
    r1,
    r2,
    b1,
    b2,
    c1,
    c2,
    arr1,
    actv,
    cotv,
    slv,
    w1v,
    w2v,
    arr2,
    hid,
    pre,
    gpre,
    acc,
    fresh,
    chunk,
    base,
    mbuf,
    ubuf,
    obuf,
    zs,
    zr,
    ss,
    sr,
    ws,
    wr,
    hs,
    hr,
    fs,
    fr,
    ts,
    tr,
    bs,
    br,
    os,
    orr,
    loc,
    outloc,
    pipe,
    ps,
    pr,
    relayed,
    based,
):
    p = lax.axis_index("path")
    z = lax.axis_index("mod")
    tokens, depth = act.shape
    cols = w1.shape[1]
    rows = depth // paths
    sub = m1.shape[1]
    modules = m1.shape[0]
    all_tokens = tokens * groups
    tile = min(cols, 256)
    scale = depth ** (-0.5)
    half = paths // 2
    partner = p + 1 - 2 * lax.rem(p, 2)
    last = groups - 1

    def ahead(step):
        return lax.rem(p + step, paths)

    def behind(step):
        return lax.rem(p + paths - step, paths)

    bufs = (actv, cotv, slv)

    def hop(i, d, s, src, block):
        to = lax.rem(z + 1, groups) if d == 0 else lax.rem(z + last, groups)
        return remote(src, bufs[i].at[block], zs.at[i, d, s], zr.at[i, d, s], (p, to))

    def can_send(d):
        return z < last if d == 0 else z > 0

    def own_send(i, d, src):
        @pl.when(can_send(d))
        def _():
            hop(i, d, 0, src, z).start()

    def block_of(d, s):
        return z - s if d == 0 else z + s

    def present(d, s):
        return z >= s if d == 0 else z + s <= last

    def relay_step(i, s):
        for d in (0, 1):
            block = block_of(d, s)

            @pl.when(present(d, s))
            def _():
                hop(i, d, s - 1, bufs[i].at[block], block).wait_recv()

            @pl.when(jnp.logical_and(present(d, s), can_send(d)))
            def _():
                hop(i, d, s, bufs[i].at[block], block).start()

    def for_blocks(s, work):
        for d in (0, 1):

            @pl.when(present(d, s))
            def _():
                work(block_of(d, s))

    def relay_finish(i):
        for s in range(groups):
            for d in (0, 1):

                @pl.when(jnp.logical_and(present(d, s), can_send(d)))
                def _():
                    block = block_of(d, s)
                    hop(i, d, s, bufs[i].at[block], block).wait_send()

    barrier = pltpu.get_barrier_semaphore()
    for step in range(1, paths):
        pl.semaphore_signal(barrier, inc=1, device_id=(ahead(step), z), device_id_type=MESH)
    for step in range(1, groups):
        pl.semaphore_signal(
            barrier, inc=1, device_id=(p, lax.rem(z + step, groups)), device_id_type=MESH
        )
    pl.semaphore_wait(barrier, paths + groups - 2)

    for i, own in enumerate((act, cot)):
        for d in (0, 1):
            own_send(i, d, own)

    def slice_copy(step):
        to = ahead(step)
        return remote(
            cot.at[:, aligned(to * rows, rows)], slv.at[z, p], ss.at[step], sr.at[step], (to, z)
        )

    def raw_copy(step):
        to = ahead(step)
        return remote(
            w2.at[aligned(to * rows, rows), :], arr2.at[p], ws.at[step], wr.at[step], (to, z)
        )

    for step in range(1, paths):
        slice_copy(step).start()
    for step in range(1, paths):
        raw_copy(step).start()

    load_act = pltpu.make_async_copy(act, actv.at[z], loc.at[0])
    load_cot = pltpu.make_async_copy(cot, cotv.at[z], loc.at[1])
    load_w1 = pltpu.make_async_copy(w1, w1v, loc.at[2])
    load_w2 = pltpu.make_async_copy(w2, w2v, loc.at[3])
    load_slice = pltpu.make_async_copy(
        cot.at[:, aligned(p * rows, rows)], slv.at[z, p], loc.at[4]
    )
    load_raw = pltpu.make_async_copy(w2.at[aligned(p * rows, rows), :], arr2.at[p], loc.at[5])
    loads = (load_act, load_w1, load_cot, load_w2, load_slice, load_raw)
    for load in loads:
        load.start()

    band = mbuf.shape[1]
    per = sub // band
    count = modules * per // 2

    def base_part(part):
        level, first_band = (1, 1, 0, 0)[part], (part % 2) * count
        m_ref, u_ref, b_ref = ((m1, u1, b1), (m2, u2, b2))[level]

        def where(i):
            i = first_band + i
            return lax.div(i, per), aligned(lax.rem(i, per) * band, band)

        def fetch(i, slot):
            m, r = where(i)
            return (
                pltpu.make_async_copy(m_ref.at[m, r, :], mbuf.at[slot], pipe.at[0, slot]),
                pltpu.make_async_copy(u_ref.at[m, r, :], ubuf.at[slot], pipe.at[1, slot]),
            )

        def put(i, slot):
            m, r = where(i)
            return pltpu.make_async_copy(obuf.at[slot], b_ref.at[m, r, :], pipe.at[2, slot])

        for copy in fetch(0, 0):
            copy.start()

        def base_step(i, carry):
            slot = lax.rem(i, 2)
            for copy in fetch(i, slot):
                copy.wait()

            @pl.when(i + 1 < count)
            def _():
                for copy in fetch(i + 1, 1 - slot):
                    copy.start()

            @pl.when(i >= 2)
            def _():
                put(i - 2, slot).wait()

            obuf[slot] = (master_factor * mbuf[slot] + moment_factor * ubuf[slot]).astype(bf16)
            put(i, slot).start()
            return carry

        with jax.named_scope("base"):
            lax.fori_loop(0, count, base_step, 0)
            for i in range(max(0, count - 2), count):
                put(i, i % 2).wait()

    for load in loads:
        load.wait()

    def forward(block):
        here = aligned(block * tokens, tokens)

        def column(n, carry):
            at = aligned(n * tile, tile)
            value = jnp.dot(actv[block], w1v[:, at], preferred_element_type=f32) * scale
            pre[here, at] = value
            hid[p, here, at] = jax.nn.silu(value).astype(bf16)
            return carry

        lax.fori_loop(0, cols // tile, column, 0)

    forward(z)
    parts = list(range(4))
    for s in range(1, groups):
        for _ in range(2 if s == 2 else 1):
            if parts:
                base_part(parts.pop(0))
        relay_step(0, s)
        for_blocks(s, forward)

    spread = half == 4

    def flip(at, bit):
        return at + bit - 2 * bit * lax.rem(lax.div(at, bit), 2)

    def source(at, j):
        if j == 0:
            return flip(at, 1)
        if spread:
            return flip(at, 2) if j == 1 else flip(at, 4) if j == 2 else flip(flip(at, 2), 4)
        return lax.rem(at + paths - 2 * j, paths)

    direct = 3 if spread else half

    def hidden_copy(j):
        to = source(p, j) if j == 0 or spread else ahead(2 * j)
        return remote(hid.at[p], hid.at[p], hs.at[j], hr.at[j], (to, z))

    def hidden_arrival(j):
        q = source(p, j)
        return remote(hid.at[q], hid.at[q], hs.at[j], hr.at[j], (partner, z))

    def hidden_half(k):
        piece = hid.at[source(p, 1 + k), pl.ds(k * (all_tokens // 2), all_tokens // 2), :]
        return remote(piece, piece, ps.at[k], pr.at[k], (source(p, 2 - k), z))

    def half_arrival(k):
        piece = hid.at[source(p, 3), pl.ds(k * (all_tokens // 2), all_tokens // 2), :]
        return remote(piece, piece, ps.at[k], pr.at[k], (partner, z))

    def pass_halves():
        for k in range(2):
            with jax.named_scope("halfwait"):
                hidden_arrival(1 + k).wait_recv()
            hidden_half(k).start()

    def hidden_onward(j):
        q = source(p, j)
        return remote(hid.at[q], hid.at[q], fs.at[j], fr.at[j], (partner, z))

    def hidden_second(j):
        q = source(partner, j)
        return remote(hid.at[q], hid.at[q], fs.at[j], fr.at[j], (partner, z))

    for j in range(direct - 1, -1, -1):
        hidden_copy(j).start()

    def backward(block):
        here = aligned(block * tokens, tokens)

        def column(n, carry):
            at = aligned(n * tile, tile)
            value = jnp.dot(cotv[block], w2v[:, at], preferred_element_type=f32) * scale
            before = pre[here, at]
            sigma = jax.nn.sigmoid(before)
            gpre[here, at] = (value * sigma * (1.0 + before * (1.0 - sigma))).astype(bf16)
            return carry

        lax.fori_loop(0, cols // tile, column, 0)

    def base_copy(level, step):
        b, c = ((b1, c1), (b2, c2))[level]
        to = lax.rem(z + step, groups)
        return remote(
            b.at[:, :, aligned(to * cols, cols)],
            c.at[:, aligned(z * sub, sub), :],
            bs.at[level, step],
            br.at[level, step],
            (p, to),
        )

    def inner(at):
        return jnp.logical_and(at > 0, at < last)

    def base_sends(level, early):
        for step in range(1, groups):
            within = jnp.logical_and(inner(z), inner(lax.rem(z + step, groups)))

            @pl.when(within if early else jnp.logical_not(within))
            def _():
                base_copy(level, step).start()

    backward(z)
    for s in range(1, groups):
        if s == last:
            while parts:
                base_part(parts.pop(0))
            base_sends(1, True)
            if spread:
                pass_halves()
        relay_step(1, s)
        if s == last:
            for step in range(1, paths):
                q = behind(step)
                remote(
                    slv.at[z, q], slv.at[z, q], ss.at[step], sr.at[step], (ahead(step), z)
                ).wait_recv()
            for d in (0, 1):
                own_send(2, d, slv.at[z])
        for_blocks(s, backward)

    def trained_copy(step):
        to = ahead(step)
        return remote(
            w1v.at[aligned(to * rows, rows), :], arr1.at[p], ts.at[step], tr.at[step], (to, z)
        )

    own_trained = pltpu.make_async_copy(w1v.at[aligned(p * rows, rows), :], arr1.at[p], loc.at[6])

    for step in list(range(1, paths)) + [0]:
        q = ahead(step)
        here = aligned(q * rows, rows)
        lhs = actv[:, :, here].reshape(all_tokens, rows)

        def column(n, carry):
            at = aligned(n * tile, tile)
            grad = lax.dot_general(
                lhs, gpre[:, at], (((0,), (0,)), ((), ())), preferred_element_type=f32
            )
            w1v[here, at] = (w1v[here, at].astype(f32) - inner_rate * (grad * scale)).astype(bf16)
            return carry

        lax.fori_loop(0, cols // tile, column, 0)
        if step == 0:
            own_trained.start()
        else:
            trained_copy(step).start()

    for s in range(1, groups):
        relay_step(2, s)

    def tell_column(sem):
        for step in range(1, groups):
            pl.semaphore_signal(
                sem, inc=1, device_id=(p, lax.rem(z + step, groups)), device_id_type=MESH
            )

    base_sends(0, True)
    tell_column(relayed)
    for j in range(1, half):
        if not spread:
            hidden_arrival(j).wait_recv()
        if spread and j == 3:
            for k in range(2):
                half_arrival(k).wait_recv()
        hidden_onward(j).start()
    with jax.named_scope("column"):
        pl.semaphore_wait(relayed, groups - 1)
    base_sends(1, False)

    hidden_arrival(0).wait_recv()
    for j in range(1, half):
        hidden_second(j).wait_recv()
    for step in range(1, paths):
        q = behind(step)
        remote(
            arr2.at[q], arr2.at[q], ws.at[step], wr.at[step], (ahead(step), z)
        ).wait_recv()

    results = (r1, r2)

    def staged(level, st, q, here):
        if level == 1:
            return arr2.at[q, here, :]
        return w2v.at[aligned((st * paths + q) * sub, sub), :]

    def out_copy(level, st, step):
        j = lax.rem(z + groups - st, groups)
        to = ahead(step)
        src = staged(level, st, to, aligned(j * sub, sub))
        dst = results[level].at[aligned(p * rows + j * sub, sub), :]
        if step == 0:
            return pltpu.make_async_copy(src, dst, outloc.at[level, st])
        return remote(src, dst, os.at[level, st, step], orr.at[level, st, step], (to, z))

    def out_arrival(level, st, step):
        j = lax.rem(z + groups - st, groups)
        q = behind(step)
        dst = results[level].at[aligned(q * rows + j * sub, sub), :]
        return remote(
            dst, dst, os.at[level, st, step], orr.at[level, st, step], (ahead(step), z)
        )

    def factor(level, m):
        taken = jnp.int32(0)
        for q in range(paths):
            taken = taken + jnp.where(routing[q, level] == m, 1, 0)
        value = jnp.float32(mean_factor)
        for k in range(2, paths + 1):
            value = jnp.where(taken == k, jnp.float32(mean_factor / k), value)
        return value

    factors = [[factor(level, m) for m in range(modules)] for level in range(2)]

    def combine(level, st, trained):
        j = lax.rem(z + groups - st, groups)
        here = aligned(j * sub, sub)
        b, c = ((b1, c1), (b2, c2))[level]
        acc[...] = jnp.zeros_like(acc)

        def add(q, carry):
            value = trained(q, here)
            for m in range(modules):
                weight = jnp.where(routing[q, level] == m, factors[level][m], 0.0)
                acc[m] = acc[m] + weight * value
            return carry

        lax.fori_loop(0, paths, add, 0)
        if st == 0:
            src = b.at[:, :, aligned(z * cols, cols)]
        else:
            src = c.at[:, here, :]
            remote(
                src, src, bs.at[level, st], br.at[level, st], (p, lax.rem(z + st, groups))
            ).wait_recv()
        load = pltpu.make_async_copy(src, base, loc.at[7])
        load.start()
        load.wait()
        for m in range(modules):
            fresh[m] = (base[m].astype(f32) + acc[m]).astype(bf16)

        def place(q, carry):
            value = fresh[routing[q, level]]
            if level == 1:
                arr2[q, here, :] = value
            else:
                w2v[aligned((st * paths + q) * sub, sub), :] = value
            return carry

        lax.fori_loop(0, paths, place, 0)
        for step in list(range(1, paths)) + [0]:
            out_copy(level, st, step).start()

    def train_second(q, carry):
        lhs = slv[:, q, :, :].reshape(all_tokens, rows)

        def column(n, carry):
            at = aligned(n * tile, tile)
            grad = lax.dot_general(
                lhs, hid[q, :, at], (((0,), (0,)), ((), ())), preferred_element_type=f32
            )
            raw = arr2[q, :, at].astype(f32)
            arr2[q, :, at] = (raw - inner_rate * (grad * scale)).astype(bf16)
            return carry

        return lax.fori_loop(0, cols // tile, column, carry)

    lax.fori_loop(0, paths, train_second, 0)

    def second(q, here):
        return arr2[q, here, :].astype(f32)

    for st in range(groups):
        combine(1, st, second)
    tell_column(based)
    with jax.named_scope("column2"):
        pl.semaphore_wait(based, groups - 1)
    base_sends(0, False)

    own_trained.wait()
    for step in range(1, paths):
        q = behind(step)
        remote(
            arr1.at[q], arr1.at[q], ts.at[step], tr.at[step], (ahead(step), z)
        ).wait_recv()

    def first(q, here):
        return chunk[q].astype(f32)

    for st in range(groups):
        j = lax.rem(z + groups - st, groups)
        load = pltpu.make_async_copy(arr1.at[:, aligned(j * sub, sub), :], chunk, loc.at[8])
        load.start()
        load.wait()
        combine(0, st, first)

    for i in range(3):
        relay_finish(i)
    for step in range(1, paths):
        slice_copy(step).wait_send()
        raw_copy(step).wait_send()
        trained_copy(step).wait_send()
    for j in range(direct):
        hidden_copy(j).wait_send()
    if spread:
        for k in range(2):
            hidden_half(k).wait_send()
    for j in range(1, half):
        hidden_onward(j).wait_send()
    for level in (1, 0):
        for step in range(1, groups):
            base_copy(level, step).wait_send()
        for st in range(groups):
            out_copy(level, st, 0).wait()
            for step in range(1, paths):
                out_copy(level, st, step).wait_send()
                out_arrival(level, st, step).wait_recv()


def deliver_kernel(block, a0, a1, o0, o1, buf, sem):
    copies = []
    for level, (a, o) in enumerate(((a0, o0), (a1, o1))):
        for i in range(a.shape[0] // block):
            here = pl.ds(i * block, block)
            slot = buf.at[level, here, :]
            copies.append(
                (
                    pltpu.make_async_copy(a.at[here, :], slot, sem.at[level, i, 0]),
                    pltpu.make_async_copy(slot, o.at[here, :], sem.at[level, i, 1]),
                )
            )
    for fetch, _ in copies:
        fetch.start()
    for fetch, put in copies:
        fetch.wait()
        put.start()
    for _, put in copies:
        put.wait()


def deliver(a0, a1):
    depth, cols = a0.shape
    block = depth // 8
    return pl.pallas_call(
        functools.partial(deliver_kernel, block),
        out_shape=(jax.ShapeDtypeStruct(a0.shape, a0.dtype),) * 2,
        in_specs=[ANY] * 2,
        out_specs=[ANY] * 2,
        scratch_shapes=[
            pltpu.VMEM((2, depth, cols), a0.dtype),
            pltpu.SemaphoreType.DMA((2, depth // block, 2)),
        ],
        compiler_params=pltpu.CompilerParams(vmem_limit_bytes=67_000_000),
        name="deliver",
    )(a0, a1)


def body(
    activations,
    cotangent,
    first_weight,
    second_weight,
    first_master,
    second_master,
    first_moment,
    second_moment,
    routing,
):
    paths = lax.axis_size("path")
    groups = lax.axis_size("mod")
    act = activations[0]
    cot = cotangent[0]
    w1 = first_weight[0]
    w2 = second_weight[0]
    tokens, depth = act.shape
    cols = w1.shape[1]
    rows = depth // paths
    modules, sub, _ = first_master.shape
    band = min(sub, 32)

    dma = pltpu.SemaphoreType.DMA
    result = jax.ShapeDtypeStruct((depth, cols), bf16)
    based = jax.ShapeDtypeStruct((modules, sub, depth), bf16)
    moved = jax.ShapeDtypeStruct((modules, rows, cols), bf16)
    outs = pl.pallas_call(
        functools.partial(round_kernel, paths, groups),
        out_shape=(
            result,
            result,
            based,
            based,
            moved,
            moved,
            jax.ShapeDtypeStruct((paths, rows, cols), bf16),
        ),
        in_specs=[ANY] * 8 + [SMEM],
        out_specs=[ANY] * 7,
        scratch_shapes=[
            pltpu.VMEM((groups, tokens, depth), bf16),
            pltpu.VMEM((groups, tokens, depth), bf16),
            pltpu.VMEM((groups, paths, tokens, rows), bf16),
            pltpu.VMEM((depth, cols), bf16),
            pltpu.VMEM((depth, cols), bf16),
            pltpu.VMEM((paths, rows, cols), bf16),
            pltpu.VMEM((paths, tokens * groups, cols), bf16),
            pltpu.VMEM((tokens * groups, cols), f32),
            pltpu.VMEM((tokens * groups, cols), bf16),
            pltpu.VMEM((modules, sub, cols), f32),
            pltpu.VMEM((modules, sub, cols), bf16),
            pltpu.VMEM((paths, sub, cols), bf16),
            pltpu.VMEM((modules, sub, cols), bf16),
            pltpu.VMEM((2, band, depth), f32),
            pltpu.VMEM((2, band, depth), f32),
            pltpu.VMEM((2, band, depth), bf16),
            dma((3, 2, groups)),
            dma((3, 2, groups)),
            dma((paths,)),
            dma((paths,)),
            dma((paths,)),
            dma((paths,)),
            dma((paths // 2,)),
            dma((paths // 2,)),
            dma((paths // 2,)),
            dma((paths // 2,)),
            dma((paths,)),
            dma((paths,)),
            dma((2, groups)),
            dma((2, groups)),
            dma((2, groups, paths)),
            dma((2, groups, paths)),
            dma((9,)),
            dma((2, groups)),
            dma((3, 2)),
            dma((2,)),
            dma((2,)),
            pltpu.SemaphoreType.REGULAR,
            pltpu.SemaphoreType.REGULAR,
        ],
        compiler_params=pltpu.CompilerParams(
            has_side_effects=True, vmem_limit_bytes=67_000_000, collective_id=0
        ),
        name="outer_round",
    )(
        act,
        cot,
        w1,
        w2,
        first_master,
        second_master,
        first_moment,
        second_moment,
        routing,
    )
    first_back, second_back = deliver(outs[0], outs[1])
    return (first_back[None], second_back[None])


def solution(mesh):
    return jax.shard_map(
        body,
        mesh=mesh,
        in_specs=(
            P("path", "mod", None),
            P("path", "mod", None),
            P("path", None, "mod"),
            P("path", None, "mod"),
            P(None, ("path", "mod"), None),
            P(None, ("path", "mod"), None),
            P(None, ("path", "mod"), None),
            P(None, ("path", "mod"), None),
            P(),
        ),
        out_specs=(P("path", None, "mod"), P("path", None, "mod")),
        check_vma=False,
    )
```
